32 devices in a mesh: tok: 8 (over z, y), rep: 4 (over x, core).
Axes of the slice: x: 2, y: 2, z: 4, core: 2. Of those that a mesh axis runs over, the one named last changes fastest.
Arguments:
- patches: bfloat16 [8192, 768], P(('tok', 'rep')), may hold values from -6 to 6
- patch_view: int32 [8192], P(('tok', 'rep')), may hold values from 0 to 511
- rays: bfloat16 [8192, 768], P(('tok', 'rep')), may hold values from -6 to 6
- ray_view: int32 [8192], P(('tok', 'rep')), may hold values from 0 to 511
- targets: float32 [3, 8192], P(None, ('tok', 'rep')), may hold values from -6 to 6
- camera: bfloat16 [512, 768], P('tok'), may hold values from -6 to 6
- slots_init: float32 [64, 768], replicated, may hold values from -6 to 6
- key_weight: bfloat16 [768, 768], P('tok'), may hold values from -0.875 to 0.875
- value_weight: bfloat16 [768, 768], P('tok'), may hold values from -0.4375 to 0.4375
- query_weight: bfloat16 [768, 768], P('tok'), may hold values from -0.21875 to 0.21875
- gru_input: bfloat16 [768, 2304], P('tok'), may hold values from -0.21875 to 0.21875
- gru_hidden: bfloat16 [768, 2304], P('tok'), may hold values from -0.21875 to 0.21875
- mix_query: bfloat16 [768, 768], P('tok'), may hold values from -0.875 to 0.875
- mix_key: bfloat16 [768, 768], P('tok'), may hold values from -0.21875 to 0.21875
- render_in: bfloat16 [768, 1536], P('tok'), may hold values from -0.21875 to 0.21875
- render_out: bfloat16 [3, 1536], P(None, 'tok'), may hold values from -0.15625 to 0.15625
Outputs:
- slots_out: float32 [64, 768], replicated
- colour: float32 [3, 8192], P(None, ('tok', 'rep'))
- loss: float32 [], replicated
- grad_render_in: float32 [768, 1536], P('tok')
- grad_render_out: float32 [3, 1536], replicated
The draws below stay inside these ranges and needn't reach their ends.
All inputs are finite; a program needn't handle non-finite values.
Results may differ from the reference program's by a relative error of at most 0.019.
Values may be sent and summed in bfloat16 or wider, within the bound.
No kernel may reach another device: no remote copies, remote signals or barrier semaphores. Data moves between devices by JAX's collectives and lax.ppermute only.
A program may use at most 128 MiB of HBM per device.

```python
import jax
import jax.numpy as jnp
from jax import lax

D = 768
H = 1536
SLOTS = 64
ITERS = 3
VIEWS = 512
TOKENS = 8192
RAYS = 8192


def set_ends(entries, key, smallest, largest):
    longest = entries.shape.index(max(entries.shape))
    spots = []
    for shift in (0, 1):
        where = [jax.random.randint(jax.random.fold_in(key, axis), (), 0, length) for axis, length in enumerate(entries.shape)]
        where[longest] = (where[longest] + shift) % entries.shape[longest]
        spots.append(tuple(where))
    return entries.at[spots[0]].set(smallest).at[spots[1]].set(largest)


def raised(array, key, source, target, blocks, factor):
    def block_of(dim):
        return (jnp.arange(array.shape[dim]) // (array.shape[dim] // blocks)).reshape((-1,) + (1,) * (array.ndim - 1 - dim))

    near = jax.random.permutation(key, blocks)[block_of(target)]
    far = (block_of(target) + blocks // 2) % blocks
    return jnp.where((block_of(source) == near) | (block_of(source) == far), factor * array, array)


def level_of(stream_key, dims, split, least, largest):
    def one(position, parts):
        draws = jax.random.uniform(jax.random.fold_in(jax.random.fold_in(stream_key, 6), position), (parts,), jnp.float32, least / len(split), largest / len(split))
        return jnp.repeat(jnp.exp(draws), dims[position] // parts).reshape((-1,) + (1,) * (len(dims) - position - 1))

    factor_of = one(*split[0])
    for cut in split[1:]:
        factor_of = factor_of * one(*cut)
    return factor_of


def gaussian(rng, extent, scale, limit, pieces=(), dtype=jnp.bfloat16):
    entries = scale * jax.random.normal(rng, extent, jnp.float32)
    if pieces:
        entries = entries * level_of(rng, extent, pieces, -0.22, 0.18)
    return jnp.clip(entries, -limit, limit).astype(dtype)


def heavy_noise(stream_key, dims, scale, most, split, heavy, kind=jnp.bfloat16):
    drawn = scale * jax.random.normal(stream_key, dims, jnp.float32)
    if split:
        drawn = drawn * level_of(stream_key, dims, split, -0.22, 0.18)
    return jnp.clip(raised(drawn, jax.random.fold_in(stream_key, 3), *heavy), -most, most).astype(kind)


def setup_inputs(seed: int = 0) -> dict:
    arg_keys = jax.random.split(jax.random.key(seed), 17)
    return {
        "patches": gaussian(arg_keys[0], (TOKENS, D), 1.0, 6.0, ((0, 32),)),
        "patch_view": set_ends(jax.random.randint(arg_keys[1], (TOKENS,), 0, VIEWS), jax.random.fold_in(arg_keys[1], 1), 0, VIEWS - 1).astype(jnp.int32),
        "rays": heavy_noise(arg_keys[2], (RAYS, D), 1.0, 6.0, ((0, 32),), (0, 1, 32, 2.75)),
        "ray_view": set_ends(jax.random.randint(arg_keys[3], (RAYS,), 0, VIEWS), jax.random.fold_in(arg_keys[3], 1), 0, VIEWS - 1).astype(jnp.int32),
        "targets": gaussian(arg_keys[4], (3, RAYS), 1.0, 6.0, ((1, 32),), jnp.float32),
        "camera": gaussian(arg_keys[5], (VIEWS, D), 1.0, 6.0, ((0, 8),)),
        "slots_init": gaussian(arg_keys[6], (SLOTS, D), 1.0, 6.0, (), jnp.float32),
        "key_weight": gaussian(arg_keys[7], (D, D), (D // 16) ** -0.5, 0.875, ((0, 8),)),
        "value_weight": gaussian(arg_keys[8], (D, D), (D // 4) ** -0.5, 0.4375, ((0, 8),)),
        "query_weight": gaussian(arg_keys[9], (D, D), D ** -0.5, 0.21875, ((0, 8),)),
        "gru_input": gaussian(arg_keys[10], (D, 3 * D), D ** -0.5, 0.21875, ((0, 8),)),
        "gru_hidden": gaussian(arg_keys[11], (D, 3 * D), D ** -0.5, 0.21875, ((0, 8),)),
        "mix_query": gaussian(arg_keys[12], (D, D), (D // 16) ** -0.5, 0.875, ((0, 8),)),
        "mix_key": gaussian(arg_keys[13], (D, D), D ** -0.5, 0.21875, ((0, 8),)),
        "render_in": gaussian(arg_keys[14], (D, H), D ** -0.5, 0.21875, ((0, 8),)),
        "render_out": gaussian(arg_keys[15], (3, H), H ** -0.5, 0.15625, ((1, 8),)),
    }


EPSILON = 1e-05
ATTN_FLOOR = 1e-08

def normalize(values):
    mean = lax.optimization_barrier(jnp.mean(values, axis=-1, keepdims=True))
    centred = values - mean
    spread = lax.optimization_barrier(jnp.mean(centred * centred, axis=-1, keepdims=True))
    return centred * lax.rsqrt(spread + EPSILON)

def slot_update(slots, update, gru_input, gru_hidden):
    width = slots.shape[1]
    from_update = jnp.dot(update.astype(jnp.bfloat16), gru_input, preferred_element_type=jnp.float32)
    from_state = jnp.dot(slots.astype(jnp.bfloat16), gru_hidden, preferred_element_type=jnp.float32)
    reset = jax.nn.sigmoid(from_update[:, :width] + from_state[:, :width])
    blend = jax.nn.sigmoid(from_update[:, width:2 * width] + from_state[:, width:2 * width])
    candidate = jnp.tanh(from_update[:, 2 * width:] + reset * from_state[:, 2 * width:])
    return (1.0 - blend) * candidate + blend * slots

def reference(patches, patch_view, rays, ray_view, targets, camera, slots_init, key_weight, value_weight, query_weight, gru_input, gru_hidden, mix_query, mix_key, render_in, render_out):
    scale = D ** (-0.5)
    patch_in = patches.astype(jnp.float32) + camera[patch_view].astype(jnp.float32)
    patch_x = normalize(patch_in).astype(jnp.bfloat16)
    keys = jnp.dot(patch_x, key_weight, preferred_element_type=jnp.float32).astype(jnp.bfloat16)
    values = jnp.dot(patch_x, value_weight, preferred_element_type=jnp.float32).astype(jnp.bfloat16)
    slots = slots_init
    for step in range(ITERS):
        query = (jnp.dot(normalize(slots).astype(jnp.bfloat16), query_weight, preferred_element_type=jnp.float32) * scale).astype(jnp.bfloat16)
        logits = jnp.dot(keys, query.T, preferred_element_type=jnp.float32)
        attn = jax.nn.softmax(logits, axis=1) + ATTN_FLOOR
        numer = jnp.dot(attn.astype(jnp.bfloat16).T, values, preferred_element_type=jnp.float32)
        denom = lax.optimization_barrier(jnp.sum(attn, axis=0))
        slots = slot_update(slots, numer / denom[:, None], gru_input, gru_hidden)
    slots_low = slots.astype(jnp.bfloat16)
    ray_in = rays.astype(jnp.float32) + camera[ray_view].astype(jnp.float32)
    ray_x = ray_in.astype(jnp.bfloat16)
    ray_query = (jnp.dot(ray_x, mix_query, preferred_element_type=jnp.float32) * scale).astype(jnp.bfloat16)
    slot_keys = jnp.dot(slots_low, mix_key, preferred_element_type=jnp.float32).astype(jnp.bfloat16)
    mix = jax.nn.softmax(jnp.dot(ray_query, slot_keys.T, preferred_element_type=jnp.float32), axis=1).astype(jnp.bfloat16)
    joined = (jnp.dot(mix, slots_low, preferred_element_type=jnp.float32) + ray_in).astype(jnp.bfloat16)
    pre = jnp.dot(joined, render_in, preferred_element_type=jnp.float32)
    hidden = jax.nn.silu(pre).astype(jnp.bfloat16)
    colour = lax.dot_general(render_out, hidden, (((1,), (1,)), ((), ())), preferred_element_type=jnp.float32)
    error = colour - targets
    loss = jnp.sum(error * error) / (3.0 * RAYS)
    dcol = (error * (2.0 / jnp.sqrt(jnp.float32(3.0 * RAYS)))).astype(jnp.bfloat16)
    grad_render_out = jnp.dot(dcol, hidden, preferred_element_type=jnp.float32)
    dhidden = jnp.dot(dcol.T, render_out, preferred_element_type=jnp.float32)
    sig = jax.nn.sigmoid(pre)
    dpre = (dhidden * (sig + pre * sig * (1.0 - sig))).astype(jnp.bfloat16)
    grad_render_in = lax.dot_general(joined, dpre, (((0,), (0,)), ((), ())), preferred_element_type=jnp.float32)
    return (slots, colour, loss, grad_render_in, grad_render_out)
```

```python
import jax
import jax.numpy as jnp
from jax import lax
from jax.sharding import PartitionSpec as P

ITERS = 3


EPSILON = 1e-05
ATTN_FLOOR = 1e-08
BOTH = ("tok", "rep")
F32 = jnp.float32
BF16 = jnp.bfloat16


def normalize(values):
    mean = jnp.mean(values, axis=-1, keepdims=True)
    centred = values - mean
    spread = jnp.mean(centred * centred, axis=-1, keepdims=True)
    return centred * lax.rsqrt(spread + EPSILON)


def dot(left, right, left_dim=1, right_dim=0):
    return lax.dot_general(
        left, right, (((left_dim,), (right_dim,)), ((), ())), preferred_element_type=F32
    )


def lookup(table, index):
    onehot = (index[:, None] == jnp.arange(table.shape[0], dtype=jnp.int32)[None, :]).astype(BF16)
    return dot(onehot, table)


def chunk_shape(shape, parts):
    rows, width = shape
    if rows % parts == 0:
        return (rows // parts, width)
    return (1, rows * width // parts)


def spread_out(chunk, axis):
    copies = lax.axis_size(axis)
    return lax.all_to_all(jnp.broadcast_to(chunk[None], (copies,) + chunk.shape), axis, 0, 0)


def sum_chunks(whole, axis, extra=None):
    copies = lax.axis_size(axis)
    pieces = whole.astype(BF16).reshape((copies,) + chunk_shape(whole.shape, copies))
    if extra is not None:
        extra = jnp.broadcast_to(extra.astype(BF16)[None], (copies,) + extra.shape)
        pieces = jnp.concatenate([pieces, extra], axis=1)
    return jnp.sum(lax.all_to_all(pieces, axis, 0, 0).astype(F32), axis=0)


def gru(slots, update, gru_input, gru_hidden):
    width = slots.shape[1]
    from_update = dot(update, gru_input)
    from_state = dot(slots.astype(BF16), gru_hidden)
    reset = jax.nn.sigmoid(from_update[:, :width] + from_state[:, :width])
    blend = jax.nn.sigmoid(from_update[:, width : 2 * width] + from_state[:, width : 2 * width])
    candidate = jnp.tanh(from_update[:, 2 * width :] + reset * from_state[:, 2 * width :])
    return (1.0 - blend) * candidate + blend * slots


def on_device(
    patches,
    patch_view,
    rays,
    ray_view,
    targets,
    camera,
    slots_init,
    key_weight,
    value_weight,
    query_weight,
    gru_input,
    gru_hidden,
    mix_query,
    mix_key,
    render_in,
    render_out,
):
    width = patches.shape[1]
    scale = width ** (-0.5)
    slot_count = slots_init.shape[0]
    toks, reps = lax.axis_size("tok"), lax.axis_size("rep")
    parts = toks * reps
    rep = lax.axis_index("rep")
    me = lax.axis_index("tok") * reps + rep

    def piece(rows):
        size = rows.shape[0] // reps
        return lax.dynamic_slice_in_dim(rows, rep * size, size, 0)

    key_piece, query_piece = piece(key_weight), piece(query_weight)
    first = jnp.concatenate(
        [key_piece, piece(value_weight), query_piece, piece(gru_input), piece(gru_hidden)], axis=1
    )
    first = lax.all_gather(first, BOTH, axis=0, tiled=True)
    second = jnp.concatenate([piece(mix_query), piece(mix_key), piece(render_in)], axis=1)

    camera_piece = piece(camera)
    rows = camera_piece.shape[0]
    table = spread_out(camera_piece, "tok").reshape(toks * rows, width)
    table = lax.all_gather(table, "rep", axis=0, tiled=True)

    def place(view):
        of_tok, of_rep = view // (rows * reps), (view // rows) % reps
        return (of_rep * toks + of_tok) * rows + view % rows

    start = normalize(slots_init).astype(BF16)
    depth = query_piece.shape[0]
    query_part = dot(lax.dynamic_slice_in_dim(start, me * depth, depth, 1), query_piece)
    query_chunk = (sum_chunks(query_part, BOTH) * scale).astype(BF16)
    colours = render_out.shape[0]
    flat = render_out.reshape(-1)
    lanes = query_chunk.shape[1]
    extra_rows = -(-flat.shape[0] // lanes)
    flat = jnp.pad(flat, (0, extra_rows * lanes - flat.shape[0])).reshape(extra_rows, lanes)
    got = spread_out(jnp.concatenate([query_chunk, flat], axis=0), BOTH)
    query = got[:, : query_chunk.shape[0]].reshape(slot_count, width)
    colour_full = got[:, query_chunk.shape[0] :].reshape(toks, reps, -1)[:, 0, : render_out.size]
    colour_full = colour_full.reshape(toks, colours, -1).transpose(1, 0, 2).reshape(colours, -1)
    reach = spread_out(dot(key_piece, query, 1, 1).astype(BF16), BOTH).reshape(width, slot_count)

    patch_x = normalize(patches.astype(F32) + lookup(table, place(patch_view))).astype(BF16)

    def gather_update(logits, source):
        attn = jax.nn.softmax(logits, axis=1) + ATTN_FLOOR
        numer = dot(attn.astype(BF16), source, 0, 0)
        denom = jnp.sum(attn, axis=0)
        chunk = chunk_shape(numer.shape, parts)
        denom = jnp.pad(denom, (0, -slot_count % chunk[1])).reshape(-1, chunk[1])
        total = sum_chunks(numer, BOTH, denom)
        denom = total[chunk[0] :].reshape(-1)[:slot_count]
        slot_of = (me * chunk[0] * chunk[1] + jnp.arange(chunk[0] * chunk[1])) // width
        slot_of = slot_of.reshape(chunk)[:, :1]
        mine = jnp.sum(jnp.where(slot_of == jnp.arange(slot_count)[None, :], denom[None, :], 0.0), axis=1)
        part = (total[: chunk[0]] / mine[:, None]).astype(BF16)
        return spread_out(part, BOTH).reshape(slot_count, width)

    seen = gather_update(dot(patch_x, reach), patch_x)

    ray_rows = rays.shape[0]
    half = ray_rows // 2
    group = jnp.concatenate(
        [
            lax.all_gather(rays[:half], "rep", axis=0),
            lax.all_gather(rays[half:], "rep", axis=0),
        ],
        axis=1,
    ).reshape(reps * ray_rows, width)
    aside = jnp.concatenate([targets, ray_view.astype(F32)[None]], axis=0)
    aside = lax.all_gather(aside, "rep", axis=1, tiled=True)
    group_targets, group_view = aside[:colours], aside[colours].astype(jnp.int32)
    ray_in = group.astype(F32) + lookup(table, place(group_view))
    ray_x = ray_in.astype(BF16)

    keys = dot(patch_x, first[:, :width]).astype(BF16)
    value_full = first[:, width : 2 * width]
    values = dot(patch_x, value_full).astype(BF16)
    reached = (dot(keys, first[:, 2 * width : 3 * width], 1, 1) * scale).astype(BF16)
    input_full = first[:, 3 * width : 6 * width]
    hidden_full = first[:, 6 * width :]
    second = lax.all_gather(second, BOTH, axis=0, tiled=True)

    slots = gru(slots_init, dot(seen, value_full).astype(BF16), input_full, hidden_full)
    for step in range(1, ITERS):
        logits = dot(reached, normalize(slots).astype(BF16), 1, 1)
        slots = gru(slots, gather_update(logits, values), input_full, hidden_full)

    slots_low = slots.astype(BF16)
    slot_keys = dot(slots_low, second[:, width : 2 * width]).astype(BF16)
    mixer = (dot(second[:, :width], slot_keys, 1, 1) * scale).astype(BF16)
    mix = jax.nn.softmax(dot(ray_x, mixer), axis=1).astype(BF16)
    joined = (dot(mix, slots_low) + ray_in).astype(BF16)

    units = render_in.shape[1] // reps
    head = lax.dynamic_slice_in_dim(second, 2 * width + rep * units, units, 1)
    colour_head = lax.dynamic_slice_in_dim(colour_full, rep * units, units, 1)
    pre = dot(joined, head)
    sig = jax.nn.sigmoid(pre)
    hidden = (pre * sig).astype(BF16)
    colour = jnp.sum(lax.all_gather(dot(colour_head, hidden, 1, 1), "rep", axis=0), axis=0)
    error = colour - group_targets
    rays_total = ray_rows * parts
    dcol = (error * (2.0 / jnp.sqrt(jnp.float32(3.0 * rays_total)))).astype(BF16)
    squared = jnp.sum(error * error)
    out_part = dot(dcol, hidden)
    dhidden = dot(dcol, colour_head, 0, 0)
    dpre = (dhidden * (sig + pre * sig * (1.0 - sig))).astype(BF16)
    grad = dot(joined, dpre, 0, 0)
    below = jnp.concatenate([out_part, jnp.broadcast_to(squared, (1, units))], axis=0)
    total = sum_chunks(grad, "tok", below)
    total = lax.all_gather(total, "rep", axis=1, tiled=True)
    mine = width // toks
    return (
        slots,
        lax.dynamic_slice_in_dim(colour, rep * ray_rows, ray_rows, 1),
        total[mine + colours, 0] / (3.0 * rays_total),
        total[:mine],
        total[mine : mine + colours],
    )


def solution(mesh):
    placed = (
        P(("tok", "rep"), None),
        P(("tok", "rep")),
        P(("tok", "rep"), None),
        P(("tok", "rep")),
        P(None, ("tok", "rep")),
        P("tok", None),
        P(),
        P("tok", None),
        P("tok", None),
        P("tok", None),
        P("tok", None),
        P("tok", None),
        P("tok", None),
        P("tok", None),
        P("tok", None),
        P(None, "tok"),
    )
    return jax.shard_map(
        on_device,
        mesh=mesh,
        in_specs=placed,
        out_specs=(P(), P(None, ("tok", "rep")), P(), P("tok", None), P()),
        check_vma=False,
    )
```

```python
import jax
import jax.numpy as jnp
from jax import lax
from jax.experimental import pallas as pl
from jax.experimental.pallas import tpu as pltpu
from jax.sharding import PartitionSpec as P

ITERS = 3


EPSILON = 1e-05
ATTN_FLOOR = 1e-08
BOTH = ("tok", "rep")
F32 = jnp.float32
BF16 = jnp.bfloat16
LANES = 128


def normalize(values):
    mean = jnp.mean(values, axis=-1, keepdims=True)
    centred = values - mean
    spread = jnp.mean(centred * centred, axis=-1, keepdims=True)
    return centred * lax.rsqrt(spread + EPSILON)


def dot(left, right, left_dim=1, right_dim=0):
    return lax.dot_general(
        left, right, (((left_dim,), (right_dim,)), ((), ())), preferred_element_type=F32
    )


def lookup(table, index):
    onehot = (index[:, None] == jnp.arange(table.shape[0], dtype=jnp.int32)[None, :]).astype(BF16)
    return dot(onehot, table)


def spread_out(chunk, axis):
    copies = lax.axis_size(axis)
    return lax.all_to_all(jnp.broadcast_to(chunk[None], (copies,) + chunk.shape), axis, 0, 0)


def sum_chunks(pieces, axis):
    return jnp.sum(lax.all_to_all(pieces.astype(BF16), axis, 0, 0).astype(F32), axis=0)


def widen(block, axis, mask, spot):
    ring = [(i, i ^ mask) for i in range(lax.axis_size(axis))]
    upper = (lax.axis_index(axis) // mask) % 2 == 1
    got = lax.ppermute(block, axis, ring)
    return jnp.stack([jnp.where(upper, got, block), jnp.where(upper, block, got)], axis=spot)


def stages(axes):
    spots = []
    for axis in axes:
        mask = lax.axis_size(axis) // 2
        while mask:
            spots.append((axis, mask))
            mask //= 2
    return spots


def double(block, axis, spot=0):
    for extra, (over, mask) in enumerate(stages((axis,))):
        block = widen(block, over, mask, spot + extra)
    return block


def after(value, *earlier):
    return lax.optimization_barrier((value,) + earlier)[0]


def pack(weights):
    reps = lax.axis_size("rep")
    size = weights[0].shape[0] // reps
    widths = [weight.shape[1] for weight in weights]
    if size % 8:
        start = lax.axis_index("rep") * size
        return jnp.concatenate(
            [lax.dynamic_slice_in_dim(weight, start, size, 0) for weight in weights], axis=1
        )

    def body(rep_ref, *refs):
        column = 0
        for source, wide in zip(refs[:-1], widths):
            refs[-1][:, column : column + wide] = source[...]
            column += wide

    return pl.pallas_call(
        body,
        grid_spec=pltpu.PrefetchScalarGridSpec(
            num_scalar_prefetch=1,
            grid=(1,),
            in_specs=[pl.BlockSpec((size, wide), lambda i, rep: (rep[0], 0)) for wide in widths],
            out_specs=pl.BlockSpec((size, sum(widths)), lambda i, rep: (0, 0)),
        ),
        out_shape=jax.ShapeDtypeStruct((size, sum(widths)), weights[0].dtype),
        name="pack",
    )(lax.axis_index("rep").reshape(1), *weights)


def gru(slots, update, gru_input, gru_hidden):
    width = slots.shape[1]
    from_update = dot(update, gru_input)
    from_state = dot(slots.astype(BF16), gru_hidden)
    reset = jax.nn.sigmoid(from_update[:, :width] + from_state[:, :width])
    blend = jax.nn.sigmoid(from_update[:, width : 2 * width] + from_state[:, width : 2 * width])
    candidate = jnp.tanh(from_update[:, 2 * width :] + reset * from_state[:, 2 * width :])
    return (1.0 - blend) * candidate + blend * slots


def on_device(
    patches,
    patch_view,
    rays,
    ray_view,
    targets,
    camera,
    slots_init,
    key_weight,
    value_weight,
    query_weight,
    gru_input,
    gru_hidden,
    mix_query,
    mix_key,
    render_in,
    render_out,
):
    width = patches.shape[1]
    scale = width ** (-0.5)
    slot_count = slots_init.shape[0]
    toks, reps = lax.axis_size("tok"), lax.axis_size("rep")
    parts = toks * reps
    rep = lax.axis_index("rep")

    def piece(rows):
        size = rows.shape[0] // reps
        return lax.dynamic_slice_in_dim(rows, rep * size, size, 0)

    first = pack([key_weight, value_weight, query_weight, gru_input, gru_hidden])
    first = lax.all_gather(first, BOTH, axis=0, tiled=True)

    table = double(spread_out(piece(camera), "tok"), "rep", 1).reshape(-1, width)

    colours = render_out.shape[0]
    of_rep = slot_count // reps
    depth = query_weight.shape[0]
    start = lax.dynamic_slice_in_dim(normalize(slots_init).astype(BF16), rep * of_rep, of_rep, 0)
    start = lax.dynamic_slice_in_dim(start, lax.axis_index("tok") * depth, depth, 1)
    flat = render_out.reshape(-1)
    extra_rows = -(-flat.shape[0] // width)
    flat = jnp.pad(flat, (0, extra_rows * width - flat.shape[0])).reshape(extra_rows, width)
    got = spread_out(jnp.concatenate([dot(start, query_weight).astype(BF16), flat], axis=0), "tok")
    query = (jnp.sum(got[:, :of_rep].astype(F32), axis=0) * scale).astype(BF16)
    colour_full = got[:, of_rep:].reshape(toks, -1)[:, : render_out.size]
    colour_full = colour_full.reshape(toks, colours, -1).transpose(1, 0, 2).reshape(colours, -1)
    reach = spread_out(dot(query, key_weight, 1, 1).astype(BF16), BOTH)
    reach = reach.reshape(toks, reps, of_rep, depth).transpose(1, 2, 0, 3).reshape(slot_count, width)

    whole_rows = slot_count % parts == 0
    patch_x = normalize(patches.astype(F32) + lookup(table, patch_view)).astype(BF16)
    ones = jnp.ones((patches.shape[0], LANES), BF16)

    def gather_update(logits, source):
        attn = jax.nn.softmax(logits, axis=1) + ATTN_FLOOR
        numer = dot(attn.astype(BF16), source, 0, 0)
        if whole_rows:
            total = sum_chunks(numer.reshape(parts, -1, numer.shape[1]), BOTH)
            part = (total[:, :width] / total[:, width : width + 1]).astype(BF16)
            return spread_out(part, BOTH).reshape(slot_count, width)
        total = spread_out(sum_chunks(numer.reshape(parts, -1), BOTH), BOTH).reshape(numer.shape)
        return (total[:, :width] / total[:, width : width + 1]).astype(BF16)

    seen = gather_update(dot(patch_x, reach, 1, 1), jnp.concatenate([patch_x, ones], axis=1))

    keys = dot(patch_x, first[:, :width]).astype(BF16)
    value_full = first[:, width : 2 * width]
    values = jnp.concatenate([dot(patch_x, value_full).astype(BF16), ones], axis=1)
    reached = (dot(keys, first[:, 2 * width : 3 * width], 1, 1) * scale).astype(BF16)
    input_full, hidden_full = first[:, 3 * width : 6 * width], first[:, 6 * width :]

    mixer_full = lax.all_gather(
        after(pack([mix_query, mix_key]), first), BOTH, axis=0, tiled=True
    )
    units = render_in.shape[1] // reps
    head = lax.dynamic_slice_in_dim(render_in, rep * units, units, 1)
    mixer = (dot(mixer_full[:, :width], mixer_full[:, width:], 1, 1) * scale).astype(BF16)

    slots = gru(slots_init, dot(seen, value_full).astype(BF16), input_full, hidden_full)
    ray_rows = rays.shape[0]
    aside = jnp.concatenate([targets, ray_view.astype(F32)[None]], axis=0)
    group, aside, head = after(rays, slots), after(aside, slots), after(head, slots)
    waiting = [stages(("rep",)), stages(("tok",))]
    spot = 0
    for step in range(1, ITERS):
        logits = dot(reached, normalize(slots).astype(BF16), 1, 1)
        last = step == ITERS - 1
        while spot < step or (last and spot < max(map(len, waiting))):
            for over, mask in waiting[0][spot : spot + 1]:
                group, aside = widen(group, over, mask, spot), widen(aside, over, mask, spot)
            for over, mask in waiting[1][spot : spot + 1]:
                head = widen(head, over, mask, spot)
            spot += 1
        seen = gather_update(logits, values)
        if last:
            seen = after(seen, mixer)
        else:
            group, aside, head = after(group, seen), after(aside, seen), after(head, seen)
        slots = gru(slots, seen, input_full, hidden_full)
    head = head.reshape(width, units)
    group = group.reshape(reps * ray_rows, width)
    aside = aside.reshape(reps, colours + 1, ray_rows)
    aside = aside.transpose(1, 0, 2).reshape(colours + 1, -1)
    group_targets, group_view = aside[:colours], aside[colours].astype(jnp.int32)
    ray_in = group.astype(F32) + lookup(table, group_view)
    ray_x = ray_in.astype(BF16)

    slots_low = slots.astype(BF16)
    mixer = dot(mixer, slots_low, 1, 1).astype(BF16)
    mix = jax.nn.softmax(dot(ray_x, mixer), axis=1).astype(BF16)
    joined = (dot(mix, slots_low) + ray_in).astype(BF16)

    colour_head = lax.dynamic_slice_in_dim(colour_full, rep * units, units, 1)
    pre = dot(joined, head)
    sig = jax.nn.sigmoid(pre)
    hidden = (pre * sig).astype(BF16)
    colour = jnp.sum(lax.all_gather(dot(colour_head, hidden, 1, 1), "rep", axis=0), axis=0)
    error = colour - group_targets
    rays_total = ray_rows * parts
    dcol = (error * (2.0 / jnp.sqrt(jnp.float32(3.0 * rays_total)))).astype(BF16)
    squared = jnp.sum(error * error)
    out_part = dot(dcol, hidden)
    dhidden = dot(dcol, colour_head, 0, 0)
    dpre = (dhidden * (sig + pre * sig * (1.0 - sig))).astype(BF16)
    grad = dot(joined, dpre, 0, 0)
    below = jnp.concatenate([out_part, jnp.broadcast_to(squared, (1, units))], axis=0).astype(BF16)
    mine = width // toks
    below = jnp.broadcast_to(below[None], (toks,) + below.shape)
    grad = jnp.concatenate([grad.astype(BF16).reshape(toks, mine, units), below], axis=1)
    total = lax.all_gather(sum_chunks(grad, "tok"), "rep", axis=1, tiled=True)
    return (
        slots,
        lax.dynamic_slice_in_dim(colour, rep * ray_rows, ray_rows, 1),
        total[mine + colours, 0] / (3.0 * rays_total),
        total[:mine],
        total[mine : mine + colours],
    )


def solution(mesh):
    placed = (
        P(("tok", "rep"), None),
        P(("tok", "rep")),
        P(("tok", "rep"), None),
        P(("tok", "rep")),
        P(None, ("tok", "rep")),
        P("tok", None),
        P(),
        P("tok", None),
        P("tok", None),
        P("tok", None),
        P("tok", None),
        P("tok", None),
        P("tok", None),
        P("tok", None),
        P("tok", None),
        P(None, "tok"),
    )
    return jax.shard_map(
        on_device,
        mesh=mesh,
        in_specs=placed,
        out_specs=(P(), P(None, ("tok", "rep")), P(), P("tok", None), P()),
        check_vma=False,
    )
```
